32 devices in a mesh: blk: 4 (over y, x), rows: 8 (over z, core).
Axes of the slice: x: 2, y: 2, z: 4, core: 2. Of those that a mesh axis runs over, the one named last changes fastest.
Arguments:
- embeddings: bfloat16 [65536, 768], P(('blk', 'rows')), may hold values from -6 to 6
- coverage: float32 [65536], P(('blk', 'rows')), may hold values from 0 to 4
- chosen_index: int32 [64], replicated, may hold values from 0 to 65535, as said below
- candidate_index: int32 [512], P('blk'), may hold values from 0 to 65535, as said below
Outputs:
- new_coverage: float32 [65536], P(('blk', 'rows'))
- gains: float32 [512], P(('blk', 'rows'))
The draws below stay inside these ranges and needn't reach their ends.
Inputs may be any that keep to these rules, and one draw needn't show every extreme that they name: `chosen_index`: the entries are distinct; the rows r * 2048 to (r + 1) * 2048 - 1 hold at most 4 of them for every r, and exactly 4 for some r. `candidate_index`: entries b * 128 to (b + 1) * 128 - 1 lie in rows b * 16384 to (b + 1) * 16384 - 1.
All inputs are finite; a program needn't handle non-finite values.
Results may differ from the reference program's by a relative error of at most 0.00035.
Values may be sent and summed in bfloat16 or wider, within the bound.
A program may use at most 64 MiB of HBM per device.

```python
import jax
import jax.numpy as jnp
from jax import lax

D = 768
ROWS_DEV = 2048
CAND_BLOCK = 128
MOST = 4
N = 65536
GROUP = 16384
CHOSEN = 64
N_BLK = 4
DEVICES = 32


def draw_chosen_index(key, part):
    key_count = jax.random.fold_in(key, 11)
    key_spot = jax.random.fold_in(key, 12)
    key_perm = jax.random.fold_in(key, 13)
    key_shuffle = jax.random.fold_in(key, 14)
    halves = DEVICES // 2
    counts_half = jax.random.randint(key_count, (halves,), 0, MOST + 1)
    spot = jax.random.randint(key_spot, (), 0, halves)
    counts_half = counts_half.at[spot].set(MOST)
    counts = jnp.stack([counts_half, MOST - counts_half], axis=1).reshape(DEVICES)
    device_keys = jax.random.split(key_perm, DEVICES)
    perms = jax.vmap(lambda kk: jax.random.permutation(kk, ROWS_DEV))(device_keys)
    picked_local = perms[:, :MOST].astype(jnp.int32)
    offsets = (jnp.arange(DEVICES, dtype=jnp.int32) * ROWS_DEV)[:, None]
    globals_rows = (picked_local + offsets).reshape(DEVICES * MOST)
    valid = (jnp.arange(MOST, dtype=jnp.int32)[None, :] < counts[:, None]).reshape(DEVICES * MOST)
    order = jnp.argsort(jnp.where(valid, 0, 1).astype(jnp.int32), stable=True)[:CHOSEN]
    selected = globals_rows[order]
    return jax.random.permutation(key_shuffle, selected).astype(jnp.int32)


def draw_candidate_index(key, part):
    key_rows = jax.random.fold_in(key, 21)
    inside = jax.random.randint(key_rows, (N_BLK, CAND_BLOCK), 0, GROUP)
    offsets = (jnp.arange(N_BLK, dtype=jnp.int32) * GROUP)[:, None]
    return (inside + offsets).reshape(N_BLK * CAND_BLOCK).astype(jnp.int32)


def steps_of(rng, dims, shards, least, largest):
    level, own = 1.0, jax.random.fold_in(rng, 6)
    for dim, parts in shards:
        draws = jnp.exp(jax.random.uniform(jax.random.fold_in(own, dim), (parts,), jnp.float32, least / len(shards), largest / len(shards)))
        level = level * jnp.repeat(draws, dims[dim] // parts).reshape([-1 if axis == dim else 1 for axis in range(len(dims))])
    return level


def normal_values(own_key, extent, scale, reach, cuts=(), kind=jnp.bfloat16):
    result = jax.random.normal(own_key, extent, jnp.float32) * scale
    if len(cuts) > 0:
        result = steps_of(own_key, extent, cuts, -0.22, 0.18) * result
    return jnp.clip(result, min=-reach, max=reach).astype(kind)


def setup_inputs(seed: int = 0) -> dict:
    arg_keys = jax.random.split(jax.random.key(seed), 5)
    embeddings = normal_values(arg_keys[0], (N, D), 1.0, 6.0, ((0, 32),))
    coverage = jnp.clip(4.0 * jax.random.uniform(arg_keys[1], (N,), jnp.float32) ** steps_of(arg_keys[1], (N,), ((0, 32),), -0.2, 0.2), 0.0, 4.0)
    chosen_index = draw_chosen_index(jax.random.fold_in(arg_keys[4], 71), 0)
    candidate_index = draw_candidate_index(jax.random.fold_in(arg_keys[4], 71), 0)
    return dict(embeddings=embeddings, coverage=coverage, chosen_index=chosen_index, candidate_index=candidate_index)


def reference(embeddings, coverage, chosen_index, candidate_index):
    scale = 1.0 / (D ** 0.5)
    chosen = embeddings[chosen_index].astype(jnp.float32)
    candidates = embeddings[candidate_index].astype(jnp.float32)
    blocks = embeddings.reshape(N // ROWS_DEV, ROWS_DEV, D)
    covers = coverage.reshape(N // ROWS_DEV, ROWS_DEV)

    def one_block(pair):
        rows_block, cover_block = pair
        rows_block = rows_block.astype(jnp.float32)
        sims = jnp.dot(rows_block, chosen.T, preferred_element_type=jnp.float32) * scale
        updated = jnp.maximum(cover_block, jnp.max(sims, axis=1))
        cand_sims = jnp.dot(rows_block, candidates.T, preferred_element_type=jnp.float32) * scale
        partial_gain = jnp.sum(jnp.maximum(cand_sims - updated[:, None], 0.0), axis=0)
        return updated, partial_gain

    updated, partial_gain = lax.map(one_block, (blocks, covers))
    return updated.reshape(N), jnp.sum(partial_gain, axis=0)
```

```python
import functools

import jax
import jax.numpy as jnp
from jax import lax
from jax.experimental import pallas as pl
from jax.experimental.pallas import tpu as pltpu
from jax.sharding import PartitionSpec as P

MOST = 4
MESH = pl.DeviceIdType.MESH
NT = (((1,), (1,)), ((), ()))


def iota(shape, dim):
    return lax.broadcasted_iota(jnp.int32, shape, dim)


def log2(n):
    assert n & (n - 1) == 0
    return n.bit_length() - 1


def kernel(
    nb, nr, per, pad,
    emb_hbm, cov_ref, chosen_ref, cand_ref,
    newcov_ref, gains_ref,
    emb, mine, pair, half, part, rows_g, pack_g, ncov, gsend, grecv,
    load_sem, pair_s, pair_r, rs_s, rs_r,
    cz_s, cb_s, cs_s, c_r, kz_s, kb_s, ks_s, k_r, g_s, g_r,
):
    nz = nr // 2
    n = nb * nr
    local, width = emb.shape
    scale = 1.0 / width**0.5
    tiles = width // 128
    nk = chosen_ref.shape[1]
    nc = cand_ref.shape[1]
    length = nr * pad
    b = lax.axis_index("blk")
    r = lax.axis_index("rows")
    z = r // 2
    c = lax.rem(r, 2)
    me = b * nr + r
    base = me * local

    pieces = load_sem.shape[0]
    step = local // pieces

    def load(i):
        sl = pl.ds(i * step, step)
        return pltpu.make_async_copy(emb_hbm.at[sl], emb.at[sl], load_sem.at[i])

    for i in range(pieces):
        load(i).start()

    barrier = pltpu.get_barrier_semaphore()

    @pl.loop(1, n)
    def _(i):
        peer = lax.rem(me + i, n)
        pl.semaphore_signal(
            barrier, inc=1, device_id=(peer // nr, lax.rem(peer, nr)), device_id_type=MESH
        )

    p = iota((length, nc), 0)
    lp, lz = log2(pad), log2(nz)
    pi = p & (pad - 1)
    pz = (p >> lp) & (nz - 1)
    pc = p >> (lp + lz)
    want = ((pz * 2 + pc) * per) + pi
    pick = (want == iota((length, nc), 1)) & (pi < per)
    cand_f = (cand_ref[...] + 1).astype(jnp.float32)
    cand_col = jnp.sum(jnp.where(pick, cand_f, 0.0), axis=1, keepdims=True)
    cand_col = cand_col.astype(jnp.int32) - 1 - base

    ll = log2(local)
    ch_row = chosen_ref[...]
    sub, lane = iota((nk, nk), 0), iota((nk, nk), 1)
    ch_col = jnp.sum(
        jnp.where(sub == lane, ch_row.astype(jnp.float32), 0.0), axis=1, keepdims=True
    ).astype(jnp.int32)
    own_row, own_col = ch_row >> ll, ch_col >> ll
    same = own_row == own_col
    rank_col = jnp.sum(
        jnp.where(same & (lane < sub), 1.0, 0.0), axis=1, keepdims=True
    ).astype(jnp.int32)
    rank_row = jnp.sum(
        jnp.where(same & (sub < lane), 1.0, 0.0), axis=0, keepdims=True
    ).astype(jnp.int32)

    col = jnp.concatenate([cand_col, ch_col - base], axis=0)
    acc = jnp.zeros((length + nk, width), jnp.float32)
    for i in range(pieces):
        load(i).wait()
        hot = (col == iota((length + nk, step), 1) + i * step).astype(jnp.float32)
        acc += jnp.dot(
            hot.astype(jnp.bfloat16),
            emb[pl.ds(i * step, step), :],
            preferred_element_type=jnp.float32,
        )
    mine[...] = acc[:length].astype(jnp.bfloat16).reshape(2, nz, pad, width)
    got = acc[length:].astype(jnp.bfloat16)

    groups = 16 // MOST
    sel_sub = iota((16, nk), 0)
    for h in range(pack_g.shape[-1] // 128):
        packed = jnp.zeros((16, 128), jnp.float32)
        for t in range(h * groups, min(tiles, (h + 1) * groups)):
            sel = (own_row == me) & (sel_sub == (t % groups) * MOST + rank_row)
            packed += jnp.dot(
                sel.astype(jnp.float32).astype(jnp.bfloat16),
                got[:, t * 128 : (t + 1) * 128],
                preferred_element_type=jnp.float32,
            )
        pack_g[b, c, z, :, h * 128 : (h + 1) * 128] = packed.astype(jnp.bfloat16)

    pl.semaphore_wait(barrier, n - 1)

    def remote(src, dst, ss, rs, pb, pz_, pc_):
        return pltpu.make_async_remote_copy(
            src_ref=src, dst_ref=dst, send_sem=ss, recv_sem=rs,
            device_id=(pb, pz_ * 2 + pc_), device_id_type=MESH,
        )

    def other(i, count, k):
        return lax.rem(i + k, count)

    class Gather:
        def __init__(self, buf, zs, bs, ss, rs):
            self.buf, self.zs, self.bs, self.ss, self.rs = buf, zs, bs, ss, rs

        def to_z(self, k):
            at = self.buf.at[b, c, z]
            return remote(at, at, self.zs.at[k], self.rs.at[b, c, z], b, other(z, nz, k), c)

        def to_b(self, zz, k):
            at = self.buf.at[b, c, zz]
            return remote(
                at, at, self.bs.at[zz, k], self.rs.at[b, c, zz], other(b, nb, k), z, c
            )

        def to_s(self, bb, zz):
            at = self.buf.at[bb, c, zz]
            return remote(at, at, self.ss.at[bb, zz], self.rs.at[bb, c, zz], b, z, 1 - c)

        def wait(self, bb, cc, zz):
            at = self.buf.at[bb, cc, zz]
            remote(at, at, self.zs.at[0], self.rs.at[bb, cc, zz], b, z, 1 - c).wait_recv()

        def start(self):
            for k in range(1, nz):
                self.to_z(k).start()
            self.spread(z)

        def spread(self, zz):
            for k in range(1, nb):
                self.to_b(zz, k).start()
            self.to_s(b, zz).start()

        def column(self):
            for k in range(1, nz):
                zz = other(z, nz, k)
                self.wait(b, c, zz)
                self.spread(zz)

        def blocks(self, k):
            bb = other(b, nb, k)
            for j in range(nz):
                zz = other(z, nz, j)
                self.wait(bb, c, zz)
                self.to_s(bb, zz).start()

        def sibling(self, bb):
            for zz in range(nz):
                self.wait(bb, 1 - c, zz)

        def drain(self):
            for k in range(1, nz):
                self.to_z(k).wait_send()
            for zz in range(nz):
                for k in range(1, nb):
                    self.to_b(zz, k).wait_send()
                for bb in range(nb):
                    self.to_s(bb, zz).wait_send()

    chosen = Gather(pack_g, cz_s, cb_s, cs_s, c_r)
    cands = Gather(rows_g, kz_s, kb_s, ks_s, k_r)

    swap = remote(mine.at[1 - c], pair, pair_s, pair_r, b, z, 1 - c)
    swap.start()
    chosen.start()
    swap.wait_recv()
    half[...] = mine[c] + pair[...]

    def scatter(k):
        to = other(z, nz, k)
        return remote(half.at[to], part.at[z], rs_s.at[k], rs_r.at[z], b, to, c)

    for k in range(1, nz):
        scatter(k).start()
    chosen.column()
    total = half[z]
    for k in range(1, nz):
        zz = other(z, nz, k)
        remote(half.at[zz], part.at[zz], rs_s.at[k], rs_r.at[zz], b, zz, c).wait_recv()
        total = total + part[zz]
    rows_g[b, c, z] = total
    cands.start()
    for k in range(1, nb):
        chosen.blocks(k)
    cands.column()
    for k in range(nb):
        chosen.sibling(other(b, nb, k))

    packs = pack_g[...].reshape(n * 16, pack_g.shape[-1])
    spot_r = own_col - ((own_col >> log2(nr)) << log2(nr))
    spot_b = own_col >> log2(nr)
    spot = ((spot_b * 2 + (spot_r & 1)) * nz + (spot_r >> 1)) * 16 + rank_col
    place = iota((nk, n * 16), 1)
    best = None
    for t in range(tiles):
        pull = (place == spot + (t % groups) * MOST).astype(jnp.float32)
        h = t // groups
        rows_t = jnp.dot(
            pull.astype(jnp.bfloat16),
            packs[:, h * 128 : (h + 1) * 128],
            preferred_element_type=jnp.float32,
        ).astype(jnp.bfloat16)
        best = rows_t if best is None else jnp.concatenate([best, rows_t], axis=1)
    span = 512
    for i in range(local // span):
        sl = pl.ds(i * span, span)
        s = lax.dot_general(best, emb[sl, :], NT, preferred_element_type=jnp.float32)
        top = jnp.max(s * scale, axis=0, keepdims=True)
        new = jnp.maximum(cov_ref[:, sl], top)
        ncov[:, sl] = new
        newcov_ref[:, sl] = new

    def send_gain(bb, rr):
        to = bb * nr + rr
        return pltpu.make_async_remote_copy(
            src_ref=gsend.at[bb], dst_ref=grecv.at[me],
            send_sem=g_s.at[to], recv_sem=g_r.at[me],
            device_id=(bb, rr), device_id_type=MESH,
        )

    def block_gain(bb):
        g = rows_g[bb].reshape(length, width)
        fold = jnp.zeros((length, 128), jnp.float32)
        for i in range(local // span):
            sl = pl.ds(i * span, span)
            s = lax.dot_general(g, emb[sl, :], NT, preferred_element_type=jnp.float32)
            x = jnp.maximum(s * scale - ncov[:, sl], 0.0)
            for j in range(span // 128):
                fold += x[:, j * 128 : (j + 1) * 128]
        return jnp.sum(fold.T, axis=0, keepdims=True)

    cands.sibling(b)
    gain = block_gain(b)
    gsend[b] = gain
    grecv[me] = gain
    for k in range(1, nr):
        send_gain(b, other(r, nr, k)).start()
    for k in range(1, nb):
        cands.blocks(k)
    for k in range(1, nb):
        bb = other(b, nb, k)
        cands.sibling(bb)
        gsend[bb] = block_gain(bb)
        for j in range(nr):
            send_gain(bb, other(r, nr, j)).start()

    swap.wait_send()
    for k in range(1, nz):
        scatter(k).wait_send()
    chosen.drain()
    cands.drain()

    @pl.loop(1, n)
    def _(i):
        src = lax.rem(me + i, n)
        pltpu.make_async_remote_copy(
            src_ref=gsend.at[b], dst_ref=grecv.at[src],
            send_sem=g_s.at[src], recv_sem=g_r.at[src],
            device_id=(src // nr, lax.rem(src, nr)), device_id_type=MESH,
        ).wait()

    total_g = jnp.sum(grecv[...].reshape(n, length), axis=0, keepdims=True)
    wide = jnp.broadcast_to(total_g, (8, length))
    at = (c * nz + z) * pad
    wide = pltpu.roll(wide, lax.rem(length - at, length), 1)
    gains_ref[...] = wide[0:1, :per]


def local_fn(nb, nr, embeddings, coverage, chosen_index, candidate_index):
    local, width = embeddings.shape
    nc = candidate_index.shape[0]
    nk = chosen_index.shape[0]
    per = nc // nr
    pad = max(per, 16)
    nz = nr // 2
    n = nb * nr
    length = nr * pad
    lanes = 128 * pl.cdiv(width // 128, 16 // MOST)
    bf, f32 = jnp.bfloat16, jnp.float32
    dma = pltpu.SemaphoreType.DMA
    vmem = pl.BlockSpec(memory_space=pltpu.VMEM)
    gather_sems = [dma((nz,)), dma((nz, nb)), dma((nb, nz)), dma((nb, 2, nz))]
    new, gains = pl.pallas_call(
        functools.partial(kernel, nb, nr, per, pad),
        out_shape=(
            jax.ShapeDtypeStruct((1, local), f32),
            jax.ShapeDtypeStruct((1, per), f32),
        ),
        in_specs=[pl.BlockSpec(memory_space=pl.ANY), vmem, vmem, vmem],
        out_specs=(vmem, vmem),
        scratch_shapes=[
            pltpu.VMEM((local, width), bf),
            pltpu.VMEM((2, nz, pad, width), bf),
            pltpu.VMEM((nz, pad, width), bf),
            pltpu.VMEM((nz, pad, width), bf),
            pltpu.VMEM((nz, pad, width), bf),
            pltpu.VMEM((nb, 2, nz, pad, width), bf),
            pltpu.VMEM((nb, 2, nz, 16, lanes), bf),
            pltpu.VMEM((1, local), f32),
            pltpu.VMEM((nb, 1, length), f32),
            pltpu.VMEM((n, 1, length), f32),
            dma((4,)), dma, dma, dma((nz,)), dma((nz,)),
            *gather_sems, *gather_sems, dma((n,)), dma((n,)),
        ],
        compiler_params=pltpu.CompilerParams(
            collective_id=0, has_side_effects=True, vmem_limit_bytes=60 * 2**20
        ),
    )(
        embeddings,
        coverage.reshape(1, local),
        chosen_index.reshape(1, nk),
        candidate_index.reshape(1, nc),
    )
    return new.reshape(local), gains.reshape(per)


def solution(mesh):
    nb, nr = mesh.shape["blk"], mesh.shape["rows"]
    placed = (P(("blk", "rows"), None), P(("blk", "rows")), P(), P("blk"))
    return jax.shard_map(
        functools.partial(local_fn, nb, nr),
        mesh=mesh,
        in_specs=placed,
        out_specs=(P(("blk", "rows")), P(("blk", "rows"))),
        check_vma=False,
    )
```

```python
import functools

import jax
import jax.numpy as jnp
from jax import lax
from jax.experimental import pallas as pl
from jax.experimental.pallas import tpu as pltpu
from jax.sharding import PartitionSpec as P

MOST = 4
MESH = pl.DeviceIdType.MESH
NT = (((1,), (1,)), ((), ()))


def iota(shape, dim):
    return lax.broadcasted_iota(jnp.int32, shape, dim)


def log2(n):
    assert n & (n - 1) == 0
    return n.bit_length() - 1


def kernel(
    nb, nr, per, pad,
    emb_hbm, cov_ref, chosen_ref, cand_ref,
    newcov_ref, gains_ref,
    emb, mine, pair, half, part, rows_g, pack_g, ncov, gsend, grecv,
    load_sem, pair_s, pair_r, rs_s, rs_r,
    cz_s, cb_s, cs_s, c_r, kz_s, kb_s, ks_s, k_r, g_s, g_r,
):
    nz = nr // 2
    n = nb * nr
    local, width = emb.shape
    scale = 1.0 / width**0.5
    tiles = width // 128
    nk = chosen_ref.shape[1]
    nc = cand_ref.shape[1]
    length = nr * pad
    group = nb * 2 * pad
    b = lax.axis_index("blk")
    r = lax.axis_index("rows")
    z = r // 2
    c = lax.rem(r, 2)
    me = b * nr + r
    base = me * local

    pieces = load_sem.shape[0]
    step = local // pieces

    def load(i):
        sl = pl.ds(i * step, step)
        return pltpu.make_async_copy(emb_hbm.at[sl], emb.at[sl], load_sem.at[i])

    for i in range(pieces):
        load(i).start()

    barrier = pltpu.get_barrier_semaphore()

    @pl.loop(1, n)
    def _(i):
        peer = lax.rem(me + i, n)
        pl.semaphore_signal(
            barrier, inc=1, device_id=(peer // nr, lax.rem(peer, nr)), device_id_type=MESH
        )

    p = iota((length, nc), 0)
    lp, lz = log2(pad), log2(nz)
    pi = p & (pad - 1)
    pz = (p >> lp) & (nz - 1)
    pc = p >> (lp + lz)
    want = ((pz * 2 + pc) * per) + pi
    pick = (want == iota((length, nc), 1)) & (pi < per)
    cand_f = (cand_ref[...] + 1).astype(jnp.float32)
    cand_col = jnp.sum(jnp.where(pick, cand_f, 0.0), axis=1, keepdims=True)
    cand_col = cand_col.astype(jnp.int32) - 1 - base

    ll = log2(local)
    ch_row = chosen_ref[...]
    sub, lane = iota((nk, nk), 0), iota((nk, nk), 1)
    ch_col = jnp.sum(
        jnp.where(sub == lane, ch_row.astype(jnp.float32), 0.0), axis=1, keepdims=True
    ).astype(jnp.int32)
    own_row, own_col = ch_row >> ll, ch_col >> ll
    same = own_row == own_col
    rank_col = jnp.sum(
        jnp.where(same & (lane < sub), 1.0, 0.0), axis=1, keepdims=True
    ).astype(jnp.int32)
    rank_row = jnp.sum(
        jnp.where(same & (sub < lane), 1.0, 0.0), axis=0, keepdims=True
    ).astype(jnp.int32)

    col = jnp.concatenate([cand_col, ch_col - base], axis=0)
    acc = jnp.zeros((length + nk, width), jnp.float32)
    for i in range(pieces):
        load(i).wait()
        hot = (col == iota((length + nk, step), 1) + i * step).astype(jnp.float32)
        acc += jnp.dot(
            hot.astype(jnp.bfloat16),
            emb[pl.ds(i * step, step), :],
            preferred_element_type=jnp.float32,
        )
    mine[...] = acc[:length].astype(jnp.bfloat16).reshape(2, nz, pad, width)
    got = acc[length:].astype(jnp.bfloat16)

    groups = 16 // MOST
    sel_sub = iota((16, nk), 0)
    for h in range(pack_g.shape[-1] // 128):
        packed = jnp.zeros((16, 128), jnp.float32)
        for t in range(h * groups, min(tiles, (h + 1) * groups)):
            sel = (own_row == me) & (sel_sub == (t % groups) * MOST + rank_row)
            packed += jnp.dot(
                sel.astype(jnp.float32).astype(jnp.bfloat16),
                got[:, t * 128 : (t + 1) * 128],
                preferred_element_type=jnp.float32,
            )
        pack_g[z, b, c, :, h * 128 : (h + 1) * 128] = packed.astype(jnp.bfloat16)

    pl.semaphore_wait(barrier, n - 1)

    def remote(src, dst, ss, rs, pb, pz_, pc_):
        return pltpu.make_async_remote_copy(
            src_ref=src, dst_ref=dst, send_sem=ss, recv_sem=rs,
            device_id=(pb, pz_ * 2 + pc_), device_id_type=MESH,
        )

    def other(i, count, k):
        out = i
        for bit in range(log2(count)):
            if (k >> bit) & 1:
                out = out + (1 - 2 * lax.rem(i // 2**bit, 2)) * 2**bit
        return out

    class Gather:
        def __init__(self, buf, zs, bs, ss, rs):
            self.buf, self.zs, self.bs, self.ss, self.rs = buf, zs, bs, ss, rs

        def to_z(self, k):
            at = self.buf.at[z, b, c]
            return remote(at, at, self.zs.at[k], self.rs.at[b, c, z], b, other(z, nz, k), c)

        def to_b(self, zz, k):
            at = self.buf.at[zz, b, c]
            return remote(
                at, at, self.bs.at[zz, k], self.rs.at[b, c, zz], other(b, nb, k), z, c
            )

        def to_s(self, bb, zz):
            at = self.buf.at[zz, bb, c]
            return remote(at, at, self.ss.at[bb, zz], self.rs.at[bb, c, zz], b, z, 1 - c)

        def wait(self, bb, cc, zz):
            at = self.buf.at[zz, bb, cc]
            remote(at, at, self.zs.at[0], self.rs.at[bb, cc, zz], b, z, 1 - c).wait_recv()

        def start(self):
            for k in range(1, nz):
                self.to_z(k).start()
            self.spread(z)

        def spread(self, zz):
            for k in range(1, nb):
                self.to_b(zz, k).start()
            self.to_s(b, zz).start()

        def hop(self, k):
            zz = other(z, nz, k)
            self.wait(b, c, zz)
            self.spread(zz)

        def across(self, zz):
            for k in range(1, nb):
                bb = other(b, nb, k)
                self.wait(bb, c, zz)
                self.to_s(bb, zz).start()

        def sibling(self, zz):
            for bb in range(nb):
                self.wait(bb, 1 - c, zz)

        def drain(self):
            for k in range(1, nz):
                self.to_z(k).wait_send()
            for zz in range(nz):
                for k in range(1, nb):
                    self.to_b(zz, k).wait_send()
                for bb in range(nb):
                    self.to_s(bb, zz).wait_send()

    chosen = Gather(pack_g, cz_s, cb_s, cs_s, c_r)
    cands = Gather(rows_g, kz_s, kb_s, ks_s, k_r)

    swap = remote(mine.at[1 - c], pair, pair_s, pair_r, b, z, 1 - c)
    swap.start()
    chosen.start()
    swap.wait_recv()
    half[...] = mine[c] + pair[...]

    def scatter(k):
        to = other(z, nz, k)
        return remote(half.at[to], part.at[z], rs_s.at[k], rs_r.at[z], b, to, c)

    for k in range(1, nz):
        scatter(k).start()
    for k in range(1, nz):
        chosen.hop(k)
    total = half[z]
    for k in range(1, nz):
        zz = other(z, nz, k)
        remote(half.at[zz], part.at[zz], rs_s.at[k], rs_r.at[zz], b, zz, c).wait_recv()
        total = total + part[zz]
    rows_g[z, b, c] = total
    cands.start()
    for k in range(nz):
        chosen.across(other(z, nz, k))
    cands.hop(1)
    for k in range(nz):
        chosen.sibling(other(z, nz, k))

    packs = pack_g[...].reshape(n * 16, pack_g.shape[-1])
    spot_r = own_col - ((own_col >> log2(nr)) << log2(nr))
    spot_b = own_col >> log2(nr)
    spot = (((spot_r >> 1) * nb + spot_b) * 2 + (spot_r & 1)) * 16 + rank_col
    place = iota((nk, n * 16), 1)
    best = None
    for t in range(tiles):
        pull = (place == spot + (t % groups) * MOST).astype(jnp.float32)
        h = t // groups
        rows_t = jnp.dot(
            pull.astype(jnp.bfloat16),
            packs[:, h * 128 : (h + 1) * 128],
            preferred_element_type=jnp.float32,
        ).astype(jnp.bfloat16)
        best = rows_t if best is None else jnp.concatenate([best, rows_t], axis=1)
    span = 512
    for i in range(local // span):
        sl = pl.ds(i * span, span)
        s = lax.dot_general(best, emb[sl, :], NT, preferred_element_type=jnp.float32)
        top = jnp.max(s * scale, axis=0, keepdims=True)
        new = jnp.maximum(cov_ref[:, sl], top)
        ncov[:, sl] = new
        newcov_ref[:, sl] = new

    def send_gain(zz, bb, cc):
        rr = zz * 2 + cc
        to = bb * nr + rr
        return pltpu.make_async_remote_copy(
            src_ref=gsend.at[zz], dst_ref=grecv.at[me],
            send_sem=g_s.at[to], recv_sem=g_r.at[me],
            device_id=(bb, rr), device_id_type=MESH,
        )

    def group_gain(zz):
        g = rows_g[zz].reshape(group, width)
        fold = jnp.zeros((group, 128), jnp.float32)
        for i in range(local // span):
            sl = pl.ds(i * span, span)
            s = lax.dot_general(g, emb[sl, :], NT, preferred_element_type=jnp.float32)
            x = jnp.maximum(s * scale - ncov[:, sl], 0.0)
            for j in range(span // 128):
                fold += x[:, j * 128 : (j + 1) * 128]
        return jnp.sum(fold.T, axis=0, keepdims=True)

    for k in range(2, nz):
        cands.hop(k)
    cands.across(z)
    for j in range(nz):
        zz = other(z, nz, j)
        if j + 1 < nz:
            cands.across(other(z, nz, j + 1))
        cands.sibling(zz)
        gain = group_gain(zz)
        gsend[zz] = gain
        if j == 0:
            grecv[me] = gain
        for k in range(nb):
            bb = other(b, nb, k)
            if j or k:
                send_gain(zz, bb, c).start()
            send_gain(zz, bb, 1 - c).start()

    swap.wait_send()
    for k in range(1, nz):
        scatter(k).wait_send()
    chosen.drain()
    cands.drain()

    @pl.loop(1, n)
    def _(i):
        src = lax.rem(me + i, n)
        pltpu.make_async_remote_copy(
            src_ref=gsend.at[z], dst_ref=grecv.at[src],
            send_sem=g_s.at[src], recv_sem=g_r.at[src],
            device_id=(src // nr, lax.rem(src, nr)), device_id_type=MESH,
        ).wait()

    total_g = jnp.sum(grecv[...].reshape(n, group), axis=0, keepdims=True)
    wide = jnp.broadcast_to(total_g, (8, group))
    at = (b * 2 + c) * pad
    wide = pltpu.roll(wide, lax.rem(group - at, group), 1)
    gains_ref[...] = wide[0:1, :per]


def local_fn(nb, nr, embeddings, coverage, chosen_index, candidate_index):
    local, width = embeddings.shape
    nc = candidate_index.shape[0]
    nk = chosen_index.shape[0]
    per = nc // nr
    pad = max(per, 16)
    nz = nr // 2
    n = nb * nr
    group = nb * 2 * pad
    lanes = 128 * pl.cdiv(width // 128, 16 // MOST)
    bf, f32 = jnp.bfloat16, jnp.float32
    dma = pltpu.SemaphoreType.DMA
    vmem = pl.BlockSpec(memory_space=pltpu.VMEM)
    gather_sems = [dma((nz,)), dma((nz, nb)), dma((nb, nz)), dma((nb, 2, nz))]
    new, gains = pl.pallas_call(
        functools.partial(kernel, nb, nr, per, pad),
        out_shape=(
            jax.ShapeDtypeStruct((1, local), f32),
            jax.ShapeDtypeStruct((1, per), f32),
        ),
        in_specs=[pl.BlockSpec(memory_space=pl.ANY), vmem, vmem, vmem],
        out_specs=(vmem, vmem),
        scratch_shapes=[
            pltpu.VMEM((local, width), bf),
            pltpu.VMEM((2, nz, pad, width), bf),
            pltpu.VMEM((nz, pad, width), bf),
            pltpu.VMEM((nz, pad, width), bf),
            pltpu.VMEM((nz, pad, width), bf),
            pltpu.VMEM((nz, nb, 2, pad, width), bf),
            pltpu.VMEM((nz, nb, 2, 16, lanes), bf),
            pltpu.VMEM((1, local), f32),
            pltpu.VMEM((nz, 1, group), f32),
            pltpu.VMEM((n, 1, group), f32),
            dma((4,)), dma, dma, dma((nz,)), dma((nz,)),
            *gather_sems, *gather_sems, dma((n,)), dma((n,)),
        ],
        compiler_params=pltpu.CompilerParams(
            collective_id=0, has_side_effects=True, vmem_limit_bytes=60 * 2**20
        ),
    )(
        embeddings,
        coverage.reshape(1, local),
        chosen_index.reshape(1, nk),
        candidate_index.reshape(1, nc),
    )
    return new.reshape(local), gains.reshape(per)


def solution(mesh):
    nb, nr = mesh.shape["blk"], mesh.shape["rows"]
    placed = (P(("blk", "rows"), None), P(("blk", "rows")), P(), P("blk"))
    return jax.shard_map(
        functools.partial(local_fn, nb, nr),
        mesh=mesh,
        in_specs=placed,
        out_specs=(P(("blk", "rows")), P(("blk", "rows"))),
        check_vma=False,
    )
```

```python
import functools

import jax
import jax.numpy as jnp
from jax import lax
from jax.experimental import pallas as pl
from jax.experimental.pallas import tpu as pltpu
from jax.sharding import PartitionSpec as P

MOST = 4
MESH = pl.DeviceIdType.MESH
NT = (((1,), (1,)), ((), ()))


def iota(shape, dim):
    return lax.broadcasted_iota(jnp.int32, shape, dim)


def log2(n):
    assert n & (n - 1) == 0
    return n.bit_length() - 1


def kernel(
    nb, nr, per, pad,
    emb_hbm, cov_ref, chosen_ref, cand_ref,
    newcov_ref, gains_ref,
    emb, mine, pair, half, part, rows_g, pack_g, ncov, gsend, grecv,
    load_sem, pair_s, pair_r, rs_s, rs_r,
    cz_s, cb_s, cs_s, c_r, kz_s, kb_s, ks_s, k_r, g_s, g_r,
):
    nz = nr // 2
    n = nb * nr
    local, width = emb.shape
    scale = 1.0 / width**0.5
    tiles = width // 128
    nk = chosen_ref.shape[1]
    nc = cand_ref.shape[1]
    length = nr * pad
    group = nb * 2 * pad
    b = lax.axis_index("blk")
    r = lax.axis_index("rows")
    z = r // 2
    c = lax.rem(r, 2)
    me = b * nr + r
    base = me * local

    pieces = load_sem.shape[0]
    step = local // pieces

    def load(i):
        sl = pl.ds(i * step, step)
        return pltpu.make_async_copy(emb_hbm.at[sl], emb.at[sl], load_sem.at[i])

    for i in range(pieces):
        load(i).start()

    barrier = pltpu.get_barrier_semaphore()

    @pl.loop(1, n)
    def _(i):
        peer = lax.rem(me + i, n)
        pl.semaphore_signal(
            barrier, inc=1, device_id=(peer // nr, lax.rem(peer, nr)), device_id_type=MESH
        )

    p = iota((length, nc), 0)
    lp, lz = log2(pad), log2(nz)
    pi = p & (pad - 1)
    pz = (p >> lp) & (nz - 1)
    pc = p >> (lp + lz)
    want = ((pz * 2 + pc) * per) + pi
    pick = (want == iota((length, nc), 1)) & (pi < per)
    cand_f = (cand_ref[...] + 1).astype(jnp.float32)
    cand_col = jnp.sum(jnp.where(pick, cand_f, 0.0), axis=1, keepdims=True)
    cand_col = cand_col.astype(jnp.int32) - 1 - base

    ll = log2(local)
    ch_row = chosen_ref[...]
    sub, lane = iota((nk, nk), 0), iota((nk, nk), 1)
    ch_col = jnp.sum(
        jnp.where(sub == lane, ch_row.astype(jnp.float32), 0.0), axis=1, keepdims=True
    ).astype(jnp.int32)
    own_row, own_col = ch_row >> ll, ch_col >> ll
    same = own_row == own_col
    rank_col = jnp.sum(
        jnp.where(same & (lane < sub), 1.0, 0.0), axis=1, keepdims=True
    ).astype(jnp.int32)
    rank_row = jnp.sum(
        jnp.where(same & (sub < lane), 1.0, 0.0), axis=0, keepdims=True
    ).astype(jnp.int32)

    col = jnp.concatenate([cand_col, ch_col - base], axis=0)
    acc = jnp.zeros((length + nk, width), jnp.float32)
    for i in range(pieces):
        load(i).wait()
        hot = (col == iota((length + nk, step), 1) + i * step).astype(jnp.float32)
        acc += jnp.dot(
            hot.astype(jnp.bfloat16),
            emb[pl.ds(i * step, step), :],
            preferred_element_type=jnp.float32,
        )
    mine[...] = acc[:length].astype(jnp.bfloat16).reshape(2, nz, pad, width)
    got = acc[length:].astype(jnp.bfloat16)

    groups = 16 // MOST
    sel_sub = iota((16, nk), 0)
    for h in range(pack_g.shape[-1] // 128):
        packed = jnp.zeros((16, 128), jnp.float32)
        for t in range(h * groups, min(tiles, (h + 1) * groups)):
            sel = (own_row == me) & (sel_sub == (t % groups) * MOST + rank_row)
            packed += jnp.dot(
                sel.astype(jnp.float32).astype(jnp.bfloat16),
                got[:, t * 128 : (t + 1) * 128],
                preferred_element_type=jnp.float32,
            )
        pack_g[z, b, c, :, h * 128 : (h + 1) * 128] = packed.astype(jnp.bfloat16)

    pl.semaphore_wait(barrier, n - 1)

    def remote(src, dst, ss, rs, pb, pz_, pc_):
        return pltpu.make_async_remote_copy(
            src_ref=src, dst_ref=dst, send_sem=ss, recv_sem=rs,
            device_id=(pb, pz_ * 2 + pc_), device_id_type=MESH,
        )

    def other(i, count, k):
        out = i
        for bit in range(log2(count)):
            if (k >> bit) & 1:
                out = out + (1 - 2 * lax.rem(i // 2**bit, 2)) * 2**bit
        return out

    class Gather:
        def __init__(self, buf, zs, bs, ss, rs):
            self.buf, self.zs, self.bs, self.ss, self.rs = buf, zs, bs, ss, rs

        def to_z(self, k):
            at = self.buf.at[z, b, c]
            return remote(at, at, self.zs.at[k], self.rs.at[b, c, z], b, other(z, nz, k), c)

        def to_b(self, zz, k):
            at = self.buf.at[zz, b, c]
            return remote(
                at, at, self.bs.at[zz, k], self.rs.at[b, c, zz], other(b, nb, k), z, c
            )

        def to_s(self, bb, zz):
            at = self.buf.at[zz, bb, c]
            return remote(at, at, self.ss.at[bb, zz], self.rs.at[bb, c, zz], b, z, 1 - c)

        def wait(self, bb, cc, zz):
            at = self.buf.at[zz, bb, cc]
            remote(at, at, self.zs.at[0], self.rs.at[bb, cc, zz], b, z, 1 - c).wait_recv()

        def start(self):
            for k in range(1, nz):
                self.to_z(k).start()
            self.spread(z)

        def spread(self, zz):
            for k in range(1, nb):
                self.to_b(zz, k).start()
            self.to_s(b, zz).start()

        def hop(self, k):
            zz = other(z, nz, k)
            self.wait(b, c, zz)
            self.spread(zz)

        def across(self, zz):
            for k in range(1, nb):
                bb = other(b, nb, k)
                self.wait(bb, c, zz)
                self.to_s(bb, zz).start()

        def sibling(self, zz):
            for bb in range(nb):
                self.wait(bb, 1 - c, zz)

        def drain(self):
            for k in range(1, nz):
                self.to_z(k).wait_send()
            for zz in range(nz):
                for k in range(1, nb):
                    self.to_b(zz, k).wait_send()
                for bb in range(nb):
                    self.to_s(bb, zz).wait_send()

    chosen = Gather(pack_g, cz_s, cb_s, cs_s, c_r)
    cands = Gather(rows_g, kz_s, kb_s, ks_s, k_r)

    swap = remote(mine.at[1 - c], pair, pair_s, pair_r, b, z, 1 - c)
    swap.start()
    chosen.start()
    swap.wait_recv()
    half[...] = mine[c] + pair[...]

    def scatter(k):
        to = other(z, nz, k)
        return remote(half.at[to], part.at[z], rs_s.at[k], rs_r.at[z], b, to, c)

    for k in range(1, nz):
        scatter(k).start()
    for k in range(1, nz):
        chosen.hop(k)
    total = half[z]
    for k in range(1, nz):
        zz = other(z, nz, k)
        remote(half.at[zz], part.at[zz], rs_s.at[k], rs_r.at[zz], b, zz, c).wait_recv()
        total = total + part[zz]
    rows_g[z, b, c] = total
    cands.start()
    for k in range(nz):
        chosen.across(other(z, nz, k))
    cands.hop(1)
    for k in range(nz):
        chosen.sibling(other(z, nz, k))

    packs = pack_g[...].reshape(n * 16, pack_g.shape[-1])
    spot_r = own_col - ((own_col >> log2(nr)) << log2(nr))
    spot_b = own_col >> log2(nr)
    spot = (((spot_r >> 1) * nb + spot_b) * 2 + (spot_r & 1)) * 16 + rank_col
    place = iota((nk, n * 16), 1)
    best = None
    for t in range(tiles):
        pull = (place == spot + (t % groups) * MOST).astype(jnp.float32)
        h = t // groups
        rows_t = jnp.dot(
            pull.astype(jnp.bfloat16),
            packs[:, h * 128 : (h + 1) * 128],
            preferred_element_type=jnp.float32,
        ).astype(jnp.bfloat16)
        best = rows_t if best is None else jnp.concatenate([best, rows_t], axis=1)
    span = 512
    for i in range(local // span):
        sl = pl.ds(i * span, span)
        s = lax.dot_general(best, emb[sl, :], NT, preferred_element_type=jnp.float32)
        top = jnp.max(s * scale, axis=0, keepdims=True)
        new = jnp.maximum(cov_ref[:, sl], top)
        newcov_ref[:, sl] = new
        for j in range(span // 128):
            row = new[:, j * 128 : (j + 1) * 128]
            ncov[pl.ds(i * span + j * 128, 128), :] = jnp.broadcast_to(row, (128, 128)).T

    def send_gain(zz, bb, cc):
        rr = zz * 2 + cc
        to = bb * nr + rr
        return pltpu.make_async_remote_copy(
            src_ref=gsend.at[zz], dst_ref=grecv.at[me],
            send_sem=g_s.at[to], recv_sem=g_r.at[me],
            device_id=(bb, rr), device_id_type=MESH,
        )

    def group_gain(zz):
        g = rows_g[zz].reshape(group, width)
        fold = [jnp.zeros((1, 128), jnp.float32)] * (group // 128)
        for i in range(local // span):
            sl = pl.ds(i * span, span)
            s = lax.dot_general(emb[sl, :], g, NT, preferred_element_type=jnp.float32)
            for j in range(group // 128):
                x = jnp.maximum(s[:, j * 128 : (j + 1) * 128] * scale - ncov[sl, :], 0.0)
                fold[j] = fold[j] + jnp.sum(x, axis=0, keepdims=True)
        return fold[0] if len(fold) == 1 else jnp.concatenate(fold, axis=1)

    for k in range(2, nz):
        cands.hop(k)
    cands.across(z)
    for j in range(nz):
        zz = other(z, nz, j)
        if j + 1 < nz:
            cands.across(other(z, nz, j + 1))
        cands.sibling(zz)
        gain = group_gain(zz)
        gsend[zz] = gain
        if j == 0:
            grecv[me] = gain
        for k in range(nb):
            bb = other(b, nb, k)
            if j or k:
                send_gain(zz, bb, c).start()
            send_gain(zz, bb, 1 - c).start()

    swap.wait_send()
    for k in range(1, nz):
        scatter(k).wait_send()
    chosen.drain()
    cands.drain()

    @pl.loop(1, n)
    def _(i):
        src = lax.rem(me + i, n)
        pltpu.make_async_remote_copy(
            src_ref=gsend.at[z], dst_ref=grecv.at[src],
            send_sem=g_s.at[src], recv_sem=g_r.at[src],
            device_id=(src // nr, lax.rem(src, nr)), device_id_type=MESH,
        ).wait()

    total_g = jnp.sum(grecv[...].reshape(n, group), axis=0, keepdims=True)
    wide = jnp.broadcast_to(total_g, (8, group))
    at = (b * 2 + c) * pad
    wide = pltpu.roll(wide, lax.rem(group - at, group), 1)
    gains_ref[...] = wide[0:1, :per]


def local_fn(nb, nr, embeddings, coverage, chosen_index, candidate_index):
    local, width = embeddings.shape
    nc = candidate_index.shape[0]
    nk = chosen_index.shape[0]
    per = nc // nr
    pad = max(per, 16)
    nz = nr // 2
    n = nb * nr
    group = nb * 2 * pad
    lanes = 128 * pl.cdiv(width // 128, 16 // MOST)
    bf, f32 = jnp.bfloat16, jnp.float32
    dma = pltpu.SemaphoreType.DMA
    vmem = pl.BlockSpec(memory_space=pltpu.VMEM)
    gather_sems = [dma((nz,)), dma((nz, nb)), dma((nb, nz)), dma((nb, 2, nz))]
    new, gains = pl.pallas_call(
        functools.partial(kernel, nb, nr, per, pad),
        out_shape=(
            jax.ShapeDtypeStruct((1, local), f32),
            jax.ShapeDtypeStruct((1, per), f32),
        ),
        in_specs=[pl.BlockSpec(memory_space=pl.ANY), vmem, vmem, vmem],
        out_specs=(vmem, vmem),
        scratch_shapes=[
            pltpu.VMEM((local, width), bf),
            pltpu.VMEM((2, nz, pad, width), bf),
            pltpu.VMEM((nz, pad, width), bf),
            pltpu.VMEM((nz, pad, width), bf),
            pltpu.VMEM((nz, pad, width), bf),
            pltpu.VMEM((nz, nb, 2, pad, width), bf),
            pltpu.VMEM((nz, nb, 2, 16, lanes), bf),
            pltpu.VMEM((local, 128), f32),
            pltpu.VMEM((nz, 1, group), f32),
            pltpu.VMEM((n, 1, group), f32),
            dma((4,)), dma, dma, dma((nz,)), dma((nz,)),
            *gather_sems, *gather_sems, dma((n,)), dma((n,)),
        ],
        compiler_params=pltpu.CompilerParams(
            collective_id=0, has_side_effects=True, vmem_limit_bytes=60 * 2**20
        ),
    )(
        embeddings,
        coverage.reshape(1, local),
        chosen_index.reshape(1, nk),
        candidate_index.reshape(1, nc),
    )
    return new.reshape(local), gains.reshape(per)


def solution(mesh):
    nb, nr = mesh.shape["blk"], mesh.shape["rows"]
    placed = (P(("blk", "rows"), None), P(("blk", "rows")), P(), P("blk"))
    return jax.shard_map(
        functools.partial(local_fn, nb, nr),
        mesh=mesh,
        in_specs=placed,
        out_specs=(P(("blk", "rows")), P(("blk", "rows"))),
        check_vma=False,
    )
```
